32 devices in a mesh: tile: 16 (over z, y, core), head: 2 (over x).
Axes of the slice: x: 2, y: 2, z: 4, core: 2. Of those that a mesh axis runs over, the one named last changes fastest.
Arguments:
- video_q: bfloat16 [8192, 3072], P('tile', 'head'), may hold values from -16 to 16
- video_k: bfloat16 [8192, 3072], P('tile', 'head'), may hold values from -16 to 16
- video_v: bfloat16 [8192, 3072], P('tile', 'head'), may hold values from -12 to 12
- text_q: bfloat16 [256, 3072], P('tile', 'head'), may hold values from -16 to 16
- text_k: bfloat16 [256, 3072], P('tile', 'head'), may hold values from -10 to 10
- text_v: bfloat16 [256, 3072], P('tile', 'head'), may hold values from -12 to 12
- video_proj: bfloat16 [3072, 3072], P('head'), may hold values from -0.109375 to 0.109375
- text_proj: bfloat16 [3072, 3072], P('head'), may hold values from -0.109375 to 0.109375
- window_mask: int32 [32, 27], P('tile'), may hold values from 0 to 1, as said below
- text_length: int32 [1], replicated, may hold values from 64 to 256
Outputs:
- video_out: bfloat16 [8192, 3072], P('tile', 'head')
- text_out: bfloat16 [256, 3072], P('tile', 'head')
The draws below stay inside these ranges and needn't reach their ends.
Inputs may be any that keep to these rules, and one draw needn't show every extreme that they name: window_mask[s, 9 a + 3 b + c] is 1 only if the tile at frame, row and column offsets a - 1, b - 1, c - 1 from tile s lies inside the grid of 2 x 4 x 4 tiles; the centre entry 13 is always 1.
All inputs are finite; a program needn't handle non-finite values.
Results may differ from the reference program's by a relative error of at most 0.013.
Values may be sent and summed in bfloat16 or wider, within the bound.
A program may use at most 320 MiB of HBM per device.

```python
import math
import jax
import jax.numpy as jnp
from jax import lax

D = 3072
HEADS = 24
HD = 128
TILE_TOK = 256
TEXT = 256
GT = 2
BH = 1
BW = 1
DW = 4
GH = 4
GW = 4
TILES_DEV = 2
TILES = 32
VTOK = 8192
N_HEAD = 2


def base_rows(key, draw_tag, row_total):
    sub_key = jax.random.fold_in(key, draw_tag)
    return jnp.clip(1.4 * jax.random.normal(sub_key, (row_total, HEADS * HD), jnp.float32), -8.4, 8.4)


def drawn(key, draw_tag, row_total):
    values = base_rows(key, draw_tag, row_total)
    return values


def draw_video_q(key, part):
    return drawn(key, 11, VTOK).astype(jnp.bfloat16)


def draw_video_k(key, part):
    return drawn(key, 12, VTOK).astype(jnp.bfloat16)


def draw_text_q(key, part):
    return drawn(key, 13, TEXT).astype(jnp.bfloat16)


def draw_window_mask(key, part):
    slot_ids = jnp.arange(TILES, dtype=jnp.int32)
    device_ids = slot_ids // TILES_DEV
    local_ids = slot_ids % TILES_DEV
    frame_ids = local_ids // (BH * BW)
    row_ids = device_ids // DW * BH + local_ids // BW % BH
    col_ids = device_ids % DW * BW + local_ids % BW
    offset = jnp.arange(27, dtype=jnp.int32)
    near_frame = frame_ids[:, None] + offset[None, :] // 9 - 1
    near_row = row_ids[:, None] + offset[None, :] // 3 % 3 - 1
    near_col = col_ids[:, None] + offset[None, :] % 3 - 1
    inside = (near_frame >= 0) & (near_frame < GT) & (near_row >= 0) & (near_row < GH) & (near_col >= 0) & (near_col < GW)
    retained = jax.random.randint(jax.random.fold_in(key, 21), (TILES, 27), 0, 5) > 0
    return (inside & (retained | (offset == 13)[None, :])).astype(jnp.int32)


def block_scale(own_key, extent, pieces, low, top_value):
    factor_of = 1.0
    for axis_at, parts in pieces:
        steps = jax.random.uniform(jax.random.fold_in(jax.random.fold_in(own_key, 6), axis_at), (parts,), jnp.float32, low / len(pieces), top_value / len(pieces))
        factor_of = factor_of * jnp.repeat(jnp.exp(steps), extent[axis_at] // parts).reshape((-1,) + (1,) * (len(extent) - 1 - axis_at))
    return factor_of


def scatter_about(own_key, extent, scale, reach, cuts=(), kind=jnp.bfloat16):
    values = scale * jax.random.normal(own_key, extent, jnp.float32)
    if cuts:
        values = values * block_scale(own_key, extent, cuts, -0.22, 0.18)
    return jnp.clip(values, -reach, reach).astype(kind)


def setup_inputs(seed: int = 0) -> dict:
    keys = jax.random.split(jax.random.key(seed), 11)
    return {
        "video_q": draw_video_q(jax.random.fold_in(keys[10], 71), 0),
        "video_k": draw_video_k(jax.random.fold_in(keys[10], 71), 0),
        "video_v": scatter_about(keys[2], (VTOK, HEADS * HD), 2.0, 12.0, ((0, 16), (1, 2))),
        "text_q": draw_text_q(jax.random.fold_in(keys[10], 71), 0),
        "text_k": scatter_about(keys[4], (TEXT, HEADS * HD), 1.7, 10.0, ((0, 16), (1, 2))),
        "text_v": scatter_about(keys[5], (TEXT, HEADS * HD), 2.0, 12.0, ((0, 16), (1, 2))),
        "video_proj": scatter_about(keys[6], (HEADS * HD, D), (HEADS * HD) ** -0.5, 0.109375, ((0, 2),)),
        "text_proj": scatter_about(keys[7], (HEADS * HD, D), (HEADS * HD) ** -0.5, 0.109375, ((0, 2),)),
        "window_mask": draw_window_mask(jax.random.fold_in(keys[10], 71), 0),
        "text_length": jax.random.randint(keys[9], (1,), TEXT // 4, TEXT + 1).astype(jnp.int32),
    }


NEG_FILL = -1e+30

def attend_tile(queries, window_keys, window_values, key_live, text_keys, text_values, text_live, score_scale):
    near_scores = jnp.einsum('qhd,khd->hqk', queries.astype(jnp.float32), window_keys.astype(jnp.float32)) * score_scale
    near_scores = jnp.where(key_live[None, None, :], near_scores, NEG_FILL)
    text_scores = jnp.einsum('qhd,khd->hqk', queries.astype(jnp.float32), text_keys.astype(jnp.float32)) * score_scale
    text_scores = jnp.where(text_live[None, None, :], text_scores, NEG_FILL)
    row_peak = jnp.maximum(lax.optimization_barrier(jnp.max(near_scores, axis=-1)), lax.optimization_barrier(jnp.max(text_scores, axis=-1)))
    near_weights = jnp.exp(near_scores - row_peak[..., None])
    text_weights = jnp.exp(text_scores - row_peak[..., None])
    weight_sum = lax.optimization_barrier(jnp.sum(near_weights, axis=-1)) + lax.optimization_barrier(jnp.sum(text_weights, axis=-1))
    near_rounded = lax.optimization_barrier(near_weights.astype(jnp.bfloat16)).astype(jnp.float32)
    text_rounded = lax.optimization_barrier(text_weights.astype(jnp.bfloat16)).astype(jnp.float32)
    weighted = jnp.einsum('hqk,khd->hqd', near_rounded, window_values.astype(jnp.float32))
    weighted = weighted + jnp.einsum('hqk,khd->hqd', text_rounded, text_values.astype(jnp.float32))
    result = weighted / weight_sum[..., None]
    return jnp.transpose(result, (1, 0, 2)).reshape(queries.shape[0], -1).astype(jnp.bfloat16)

def project_groups(attended, weight):
    row_total = attended.shape[0]
    group_width = attended.shape[1] // N_HEAD
    grouped = jnp.transpose(attended.reshape(row_total, N_HEAD, group_width), (1, 0, 2))
    weight_groups = weight.reshape(N_HEAD, group_width, weight.shape[1])

    def add_group(running_sum, group_pair):
        partial_sum = jnp.dot(group_pair[0], group_pair[1], preferred_element_type=jnp.float32).astype(jnp.bfloat16)
        partial_sum = lax.optimization_barrier(partial_sum)
        return (running_sum + partial_sum.astype(jnp.float32), None)
    running_sum, unused_out = lax.scan(add_group, jnp.zeros((row_total, weight.shape[1]), jnp.float32), (grouped, weight_groups))
    return running_sum.astype(jnp.bfloat16)

def reference(video_q, video_k, video_v, text_q, text_k, text_v, video_proj, text_proj, window_mask, text_length):
    score_scale = 1.0 / math.sqrt(HD)
    slot_ids = jnp.arange(TILES, dtype=jnp.int32)
    device_ids = slot_ids // TILES_DEV
    local_ids = slot_ids % TILES_DEV
    frame_ids = local_ids // (BH * BW)
    row_ids = device_ids // DW * BH + local_ids // BW % BH
    col_ids = device_ids % DW * BW + local_ids % BW
    offsets = jnp.arange(3, dtype=jnp.int32) - 1
    frame_grid = jnp.broadcast_to(jnp.arange(GT, dtype=jnp.int32)[None, :, None, None], (TILES, GT, 3, 3))
    row_grid = jnp.broadcast_to(jnp.clip(row_ids[:, None, None, None] + offsets[None, None, :, None], 0, GH - 1), (TILES, GT, 3, 3))
    col_grid = jnp.broadcast_to(jnp.clip(col_ids[:, None, None, None] + offsets[None, None, None, :], 0, GW - 1), (TILES, GT, 3, 3))
    neighbour_slots = (row_grid // BH * DW + col_grid // BW) * TILES_DEV + (frame_grid * BH + row_grid % BH) * BW + col_grid % BW
    neighbour_slots = neighbour_slots.reshape(TILES, GT * 9).astype(jnp.int32)
    frame_gap = frame_grid - frame_ids[:, None, None, None] + 1
    mask_column = jnp.clip(frame_gap, 0, 2) * 9 + jnp.broadcast_to((offsets[None, None, :, None] + 1) * 3 + offsets[None, None, None, :] + 1, (TILES, GT, 3, 3))
    mask_column = mask_column.reshape(TILES, GT * 9).astype(jnp.int32)
    tile_live = (jnp.take_along_axis(window_mask, mask_column, axis=1) > 0) & (jnp.abs(frame_gap - 1) <= 1).reshape(TILES, GT * 9)
    tiled_keys = video_k.reshape(TILES, TILE_TOK, HEADS, HD)
    tiled_values = video_v.reshape(TILES, TILE_TOK, HEADS, HD)
    tiled_queries = video_q.reshape(TILES, TILE_TOK, HEADS, HD)
    text_keys = text_k.reshape(TEXT, HEADS, HD)
    text_values = text_v.reshape(TEXT, HEADS, HD)
    text_live = jnp.arange(TEXT, dtype=jnp.int32) < text_length[0]

    def one_tile(slot_index):
        near_keys = tiled_keys[neighbour_slots[slot_index]].reshape(GT * 9 * TILE_TOK, HEADS, HD)
        near_values = tiled_values[neighbour_slots[slot_index]].reshape(GT * 9 * TILE_TOK, HEADS, HD)
        key_live = jnp.repeat(tile_live[slot_index], TILE_TOK)
        return attend_tile(tiled_queries[slot_index], near_keys, near_values, key_live, text_keys, text_values, text_live, score_scale)
    video_attn = lax.map(one_tile, slot_ids).reshape(VTOK, HEADS * HD)

    def head_major(array, count):
        return jnp.transpose(array.reshape(count, HEADS, HD), (1, 0, 2))

    def one_head(head_parts):
        head_query, head_keys, head_values, head_text_keys, head_text_values = head_parts
        near_scores = jnp.dot(head_query, head_keys.T, preferred_element_type=jnp.float32) * score_scale
        text_scores = jnp.dot(head_query, head_text_keys.T, preferred_element_type=jnp.float32) * score_scale
        text_scores = jnp.where(text_live[None, :], text_scores, NEG_FILL)
        row_peak = jnp.maximum(lax.optimization_barrier(jnp.max(near_scores, axis=-1)), lax.optimization_barrier(jnp.max(text_scores, axis=-1)))
        near_weights = jnp.exp(near_scores - row_peak[:, None])
        text_weights = jnp.exp(text_scores - row_peak[:, None])
        weight_sum = lax.optimization_barrier(jnp.sum(near_weights, axis=-1)) + lax.optimization_barrier(jnp.sum(text_weights, axis=-1))
        weighted = jnp.dot(near_weights, head_values.astype(jnp.float32), precision=lax.Precision.HIGHEST)
        weighted = weighted + jnp.dot(text_weights, head_text_values.astype(jnp.float32), precision=lax.Precision.HIGHEST)
        return weighted / weight_sum[:, None]
    text_heads = lax.map(one_head, (head_major(text_q, TEXT), head_major(video_k, VTOK), head_major(video_v, VTOK), head_major(text_k, TEXT), head_major(text_v, TEXT)))
    text_attn = jnp.transpose(text_heads, (1, 0, 2)).reshape(TEXT, HEADS * HD).astype(jnp.bfloat16)
    return (project_groups(video_attn, video_proj), project_groups(text_attn, text_proj))
```

```python
import functools
import math

import jax
import jax.numpy as jnp
from jax import lax
from jax.experimental import pallas as pl
from jax.experimental.pallas import tpu as pltpu
from jax.sharding import PartitionSpec as P

HD = 128
TILE_TOK = 256
GT = 2
DH = 4
NEG_FILL = -1e30
SCALE = 1.0 / math.sqrt(HD)
SCALE2 = SCALE * math.log2(math.e)
CHUNKS = 4


GROUPS = (
    ((0, 0), (-1, 0), (1, 0)),
    ((0, -1), (0, 1)),
    ((-1, -1), (-1, 1), (1, -1), (1, 1)),
)
NEAR = tuple(gap for group in GROUPS for gap in group)

NT = (((1,), (1,)), ((), ()))


def dot_nt(a, b):
    return lax.dot_general(a, b, NT, preferred_element_type=jnp.float32)


def with_ones(values):
    return jnp.concatenate([values, jnp.ones_like(values)], axis=1)


def video_kernel(mask_ref, length_ref, q_ref, *refs):
    near_refs = dict(zip(NEAR, refs[:9]))
    tk_ref, tv_ref, out_ref = refs[9:]
    tiles = q_ref.shape[0] // TILE_TOK
    queries = [q_ref[t * TILE_TOK : (t + 1) * TILE_TOK, :] for t in range(tiles)]
    peak = [None] * tiles
    acc = [None] * tiles
    for number, group in enumerate(GROUPS):
        values = [with_ones(near_refs[gap][1]) for gap in group]
        last = number == len(GROUPS) - 1
        if last:
            text_values = with_ones(tv_ref[...])
        for t in range(tiles):
            parts = []
            maxima = []
            for gap, value in zip(group, values):
                scores = dot_nt(queries[t], near_refs[gap][0])
                for f in range(GT):
                    slot = 9 * (f - t + 1) + 3 * (gap[0] + 1) + gap[1] + 1
                    bias = jnp.where(mask_ref[t, slot] > 0, 0.0, NEG_FILL).astype(jnp.float32)
                    piece = scores[:, f * TILE_TOK : (f + 1) * TILE_TOK]
                    maxima.append(jnp.max(piece, axis=1, keepdims=True) + bias)
                    parts.append((piece, bias, value, f))
            if last:
                scores = dot_nt(queries[t], tk_ref[...])
                live = lax.broadcasted_iota(jnp.int32, scores.shape, 1) < length_ref[0]
                scores = jnp.where(live, scores, NEG_FILL)
                maxima.append(jnp.max(scores, axis=1, keepdims=True))
            new_peak = functools.reduce(jnp.maximum, maxima)
            if peak[t] is not None:
                new_peak = jnp.maximum(peak[t], new_peak)
            shift = new_peak * SCALE2
            total = None
            for at in range(0, len(parts), GT):
                weights = [
                    jnp.exp2(piece * SCALE2 - (shift - bias)).astype(jnp.bfloat16)
                    for piece, bias, _, _ in parts[at : at + GT]
                ]
                term = jnp.dot(
                    jnp.concatenate(weights, axis=1),
                    parts[at][2],
                    preferred_element_type=jnp.float32,
                )
                total = term if total is None else total + term
            if last:
                weights = jnp.exp2(scores * SCALE2 - shift).astype(jnp.bfloat16)
                total = total + jnp.dot(weights, text_values, preferred_element_type=jnp.float32)
            if acc[t] is None:
                acc[t] = total
            else:
                acc[t] = acc[t] * jnp.exp2(peak[t] * SCALE2 - shift) + total
            peak[t] = new_peak
    for t in range(tiles):
        out_ref[t * TILE_TOK : (t + 1) * TILE_TOK, :] = (
            acc[t][:, :HD] / acc[t][:, HD : HD + 1]
        ).astype(jnp.bfloat16)


def video_attention(mask, length, video_q, near, text_k, text_v, first_head, heads):
    rows = video_q.shape[0]
    text = text_k.shape[0]
    smem = pl.BlockSpec(memory_space=pltpu.SMEM)
    own = pl.BlockSpec((rows, HD), lambda h: (0, first_head + h))
    block = pl.BlockSpec((2, rows, HD), lambda h: (0, 0, h))
    token = pl.BlockSpec((text, HD), lambda h: (0, first_head + h))
    keys = 9 * rows + text
    return pl.pallas_call(
        video_kernel,
        grid=(heads,),
        in_specs=[smem, smem, own] + [block] * 9 + [token] * 2,
        out_specs=pl.BlockSpec((rows, HD), lambda h: (0, h)),
        out_shape=jax.ShapeDtypeStruct((rows, heads * HD), jnp.bfloat16),
        compiler_params=pltpu.CompilerParams(vmem_limit_bytes=56 * 1024 * 1024),
        cost_estimate=pl.CostEstimate(
            flops=8 * heads * rows * keys * HD,
            bytes_accessed=heads * keys * HD * 4,
            transcendentals=heads * rows * keys,
        ),
        name="video_attention",
    )(mask, length, video_q, *[near[gap] for gap in NEAR], text_k, text_v)


def text_kernel(first_ref, length_ref, q_ref, k_ref, v_ref, tk_ref, tv_ref, out_ref, lse_ref):
    head = pl.program_id(0)
    queries = q_ref[...]
    scores = dot_nt(queries, k_ref[...])
    own = dot_nt(queries, tk_ref[...])
    live = first_ref[0] + lax.broadcasted_iota(jnp.int32, own.shape, 1) < length_ref[0]
    own = jnp.where(live, own, NEG_FILL)
    peak = jnp.maximum(
        jnp.max(scores, axis=1, keepdims=True), jnp.max(own, axis=1, keepdims=True)
    )
    weights = jnp.exp2((scores - peak) * SCALE2)
    own_weights = jnp.exp2((own - peak) * SCALE2)
    total = jnp.sum(weights, axis=1, keepdims=True) + jnp.sum(own_weights, axis=1, keepdims=True)
    acc = jnp.dot(weights.astype(jnp.bfloat16), v_ref[...], preferred_element_type=jnp.float32)
    acc = acc + jnp.dot(
        own_weights.astype(jnp.bfloat16), tv_ref[...], preferred_element_type=jnp.float32
    )
    out_ref[...] = (acc / total).astype(jnp.bfloat16)
    lse = peak * SCALE + jnp.log(total)

    @pl.when(head == 0)
    def _():
        lse_ref[...] = jnp.zeros_like(lse_ref)

    lane = lax.broadcasted_iota(jnp.int32, lse_ref.shape, 1)
    lse_ref[...] = jnp.where(lane == head, lse, lse_ref[...])


def text_attention(first, length, text_q, video_k, video_v, text_k, text_v):
    rows, width = video_k.shape
    text = text_q.shape[0]
    heads = width // HD
    smem = pl.BlockSpec(memory_space=pltpu.SMEM)

    def column(count):
        return pl.BlockSpec((count, HD), lambda h: (0, h))

    return pl.pallas_call(
        text_kernel,
        grid=(heads,),
        in_specs=[smem, smem, column(text), column(rows), column(rows)]
        + [column(text_k.shape[0])] * 2,
        out_specs=[column(text), pl.BlockSpec((text, HD), lambda h: (0, 0))],
        out_shape=[
            jax.ShapeDtypeStruct((text, width), jnp.bfloat16),
            jax.ShapeDtypeStruct((text, HD), jnp.float32),
        ],
        cost_estimate=pl.CostEstimate(
            flops=8 * heads * rows * text * HD,
            bytes_accessed=4 * rows * width,
            transcendentals=heads * rows * text,
        ),
        name="text_attention",
    )(first, length, text_q, video_k, video_v, text_k, text_v)


def from_gap(block, row_gap, col_gap):
    across = lax.axis_size("tile") // DH
    route = []
    for t in range(lax.axis_size("tile")):
        row, col = t // across + row_gap, t % across + col_gap
        if 0 <= row < DH and 0 <= col < across:
            route.append((row * across + col, t))
    return lax.ppermute(block, "tile", route)


def halo(own):
    near = {(0, 0): own}
    for gap in (-1, 1):
        near[gap, 0] = from_gap(own, gap, 0)
    for gap in (-1, 1):
        near[0, gap] = from_gap(own, 0, gap)
    for row_gap in (-1, 1):
        for gap in (-1, 1):
            near[row_gap, gap] = from_gap(near[row_gap, 0], 0, gap)
    return near


def per_device(
    video_q,
    video_k,
    video_v,
    text_q,
    text_k,
    text_v,
    video_proj,
    text_proj,
    window_mask,
    text_length,
):
    rows, width = video_q.shape
    heads = width // HD
    local = text_q.shape[0]
    devices = lax.axis_size("tile")
    groups = lax.axis_size("head")
    chunks = max(c for c in range(1, CHUNKS + 1) if heads % c == 0)
    step = heads // chunks

    text = lax.all_gather(jnp.stack([text_q, text_k, text_v]), "tile", axis=1, tiled=True)
    nears = []
    for c in range(chunks):
        part = slice(c * step * HD, (c + 1) * step * HD)
        nears.append(halo(jnp.stack([video_k[:, part], video_v[:, part]])))

    first = (lax.axis_index("tile") * local).astype(jnp.int32).reshape(1)
    text_part, text_lse = text_attention(
        first, text_length, text[0], video_k, video_v, text_k, text_v
    )
    text_part = lax.all_to_all(
        text_part.reshape(devices, local, width), "tile", split_axis=0, concat_axis=0
    )
    text_lse = lax.all_to_all(
        text_lse.reshape(devices, local, HD), "tile", split_axis=0, concat_axis=0
    )[:, :, :heads]
    share = jax.nn.softmax(text_lse, axis=0)
    text_attn = jnp.sum(
        share[..., None] * text_part.reshape(devices, local, heads, HD).astype(jnp.float32), axis=0
    )
    text_attn = text_attn.reshape(local, width).astype(jnp.bfloat16)

    results = [
        video_attention(
            window_mask, text_length, video_q, near, text[1], text[2], c * step, step
        )
        for c, near in enumerate(nears)
    ]
    video_attn = jnp.concatenate(results, axis=1)
    return (
        project(video_attn, video_proj, groups),
        project(text_attn, text_proj, groups),
    )


def project(attn, proj, groups):
    if groups != 2:
        part = jnp.dot(attn, proj, preferred_element_type=jnp.float32).astype(jnp.bfloat16)
        return lax.psum_scatter(part, "head", scatter_dimension=1, tiled=True)
    half = proj.shape[1] // groups
    me = lax.axis_index("head")
    theirs = lax.dynamic_slice_in_dim(proj, (1 - me) * half, half, 1)
    mine = lax.dynamic_slice_in_dim(proj, me * half, half, 1)
    away = jnp.dot(attn, theirs, preferred_element_type=jnp.float32).astype(jnp.bfloat16)
    arrived = lax.ppermute(away, "head", [(0, 1), (1, 0)])
    home = jnp.dot(attn, mine, preferred_element_type=jnp.float32).astype(jnp.bfloat16)
    return (home.astype(jnp.float32) + arrived.astype(jnp.float32)).astype(jnp.bfloat16)


def solution(mesh):
    placed = (P("tile", "head"),) * 6 + (P("head", None),) * 2 + (P("tile", None), P())
    return jax.shard_map(
        per_device,
        mesh=mesh,
        in_specs=placed,
        out_specs=(P("tile", "head"), P("tile", "head")),
        check_vma=False,
    )
```
